32 devices in a mesh: high: 4 (over z), low: 2 (over x), unit: 4 (over y, core).
Axes of the slice: x: 2, y: 2, z: 4, core: 2. Of those that a mesh axis runs over, the one named last changes fastest.
Arguments:
- wave_parts: float32 [8, 32, 128, 128], P('unit', ('high', 'low')), parts along dimension 0, may hold values from -6 to 6
- level_table: float32 [128, 128, 128], P(('unit', 'high', 'low')), parts along dimension 0, may hold values from -2 to 2
- phase_angles: float32 [8, 128], P('unit'), parts along dimension 0, may hold values from 0.3 to 1.2
- mix_angles: float32 [8, 4], P('unit'), parts along dimension 0, may hold values from 0.3 to 1.2
Outputs:
- result_parts: float32 [8, 32, 128, 128], P('unit', ('high', 'low')), parts along dimension 0
The draws below stay inside these ranges and needn't reach their ends.
There are 4 independent parts, one for each index of `unit`. The reference program is written for one: setup_inputs(seed, part) draws one part's arguments, and reference() takes and returns one part's arrays. A program takes and returns all parts, laid end to end along the dimension named above; each array names one. Nothing has to cross between parts.
All inputs are finite; a program needn't handle non-finite values.
Results may differ from the reference program's by a relative error of at most 0.0003.
Values sent between devices are 32-bit elements.
A program may use at most 64 MiB of HBM per device.

```python
import jax
import jax.numpy as jnp
from jax import lax

BLOCKS_DEV = 4
ROWS = 128
LANES = 128
BLOCKS = 32
LAYERS = 2
N_HIGH = 4
N_LOW = 2


def steps_of(own_key, dims, shards, least, largest):
    loudness, own = 1.0, jax.random.fold_in(own_key, 6)
    for position, blocks in shards:
        steps = jnp.exp(jax.random.uniform(jax.random.fold_in(own, position), (blocks,), jnp.float32, least / len(shards), largest / len(shards)))
        loudness = loudness * jnp.repeat(steps, dims[position] // blocks).reshape([-1 if axis == position else 1 for axis in range(len(dims))])
    return loudness


def noise(key, extent, scale, limit, cuts=(), kind=jnp.bfloat16):
    entries = jax.random.normal(key, extent, jnp.float32) * scale
    if len(cuts) > 0:
        entries = steps_of(key, extent, cuts, -0.22, 0.18) * entries
    return jnp.clip(entries, min=-limit, max=limit).astype(kind)


def setup_inputs(seed: int = 0, part: int = 0) -> dict:
    keys = jax.random.split(jax.random.key(seed), 5)
    own_keys = jax.random.split(jax.random.fold_in(keys[4], part), 5)
    wave_parts = noise(own_keys[0], (2, BLOCKS, ROWS, LANES), 1.0, 6.0, ((1, 8),), jnp.float32)
    level_table = jnp.clip(jax.random.uniform(own_keys[1], (BLOCKS, ROWS, LANES), jnp.float32, -2.0, 2.0) * steps_of(own_keys[1], (BLOCKS, ROWS, LANES), ((0, 8),), -0.4, 0.0), -2.0, 2.0)
    phase_angles = jnp.clip(jax.random.uniform(own_keys[2], (LAYERS, LANES), jnp.float32, 0.3, 1.2), 0.3, 1.2)
    mix_angles = jnp.clip(jax.random.uniform(own_keys[3], (LAYERS, 4), jnp.float32, 0.3, 1.2), 0.3, 1.2)
    return dict(wave_parts=wave_parts, level_table=level_table, phase_angles=phase_angles, mix_angles=mix_angles)


def count_bits(values, count):
    places = jnp.arange(count.bit_length() - 1, dtype=jnp.int32)
    return jnp.sum((values[..., None] >> places) & 1, axis=-1)


def mix_table(count, angle):
    rank = jnp.arange(count, dtype=jnp.int32)
    apart = count_bits(rank[:, None] ^ rank[None, :], count)
    bits = count.bit_length() - 1
    size = jnp.cos(angle) ** (bits - apart).astype(jnp.float32) * jnp.sin(angle) ** apart.astype(jnp.float32)
    real_sign = jnp.where(apart % 4 == 0, 1.0, jnp.where(apart % 4 == 2, -1.0, 0.0)).astype(jnp.float32)
    imag_sign = jnp.where(apart % 4 == 1, -1.0, jnp.where(apart % 4 == 3, 1.0, 0.0)).astype(jnp.float32)
    return size * real_sign, size * imag_sign


def turn_dim(values, dim, angle):
    real_part, imag_part = mix_table(values.shape[dim], angle)
    def times(table):
        moved = jnp.tensordot(values, table, axes=([dim], [0]), precision=lax.Precision.HIGHEST)
        return jnp.moveaxis(moved, -1, dim)
    by_real = times(real_part)
    by_imag = times(imag_part)
    return jnp.stack([by_real[0] - by_imag[1], by_real[1] + by_imag[0]])


def turn_phase(values, levels, angle):
    turn = angle * levels
    return jnp.stack([values[0] * jnp.cos(turn) + values[1] * jnp.sin(turn), values[1] * jnp.cos(turn) - values[0] * jnp.sin(turn)])


def reference(wave_parts, level_table, phase_angles, mix_angles):
    values = wave_parts
    for layer in range(LAYERS):
        values = turn_phase(values, level_table, phase_angles[layer])
        values = turn_dim(values, 3, mix_angles[layer, 0])
        values = turn_dim(values, 2, mix_angles[layer, 1])
        parts = values.reshape(2, N_HIGH, N_LOW, BLOCKS_DEV, ROWS, LANES)
        parts = turn_dim(parts, 1, mix_angles[layer, 2])
        parts = turn_dim(parts, 2, mix_angles[layer, 3])
        parts = turn_dim(parts, 3, mix_angles[layer, 2])
        values = parts.reshape(values.shape)
    return values
```

```python
import functools
import math

import jax
import jax.numpy as jnp
from jax import lax
from jax.experimental import pallas as pl
from jax.experimental.pallas import tpu as pltpu
from jax.sharding import PartitionSpec as P

LAYERS = 2
MESH = pl.DeviceIdType.MESH
CHUNKS = 4


def cos_sin(x):
    turns = jnp.floor(x * (0.5 / math.pi) + 0.5)
    r = x - turns * 6.28125
    r = r - turns * (2 * math.pi - 6.28125)
    y = r * r
    sine = jnp.full_like(y, -1.0 / math.factorial(19))
    for n in range(17, 0, -2):
        sine = sine * y + (-1.0) ** (n // 2) / math.factorial(n)
    cosine = jnp.full_like(y, -1.0 / math.factorial(18))
    for n in range(16, -1, -2):
        cosine = cosine * y + (-1.0) ** (n // 2) / math.factorial(n)
    return cosine, sine * r


def bits_of(count):
    return count.bit_length() - 1


def popcount(values, bits):
    total = values & 1
    for k in range(1, bits):
        total = total + ((values >> k) & 1)
    return total


def rotation(size, c, s, transposed):
    out = lax.broadcasted_iota(jnp.int32, (size, size), 1 if transposed else 0)
    inn = lax.broadcasted_iota(jnp.int32, (size, size), 0 if transposed else 1)
    differ = out ^ inn
    c = jnp.broadcast_to(c, (size, size))
    s = jnp.broadcast_to(s, (size, size))
    table = None
    for k in range(bits_of(size)):
        turned = jnp.where(((out >> k) & 1) == 1, -s, s)
        factor = jnp.where(((differ >> k) & 1) == 1, turned, c)
        table = factor if table is None else table * factor
    return table


def rotate_list(parts, bit, c, s):
    fresh = list(parts)
    for n in range(len(parts)):
        if not n >> bit & 1:
            m = n | 1 << bit
            fresh[n] = c * parts[n] + s * parts[m]
            fresh[m] = c * parts[m] - s * parts[n]
    return fresh


def mm(a, b):
    return lax.dot_general(
        a,
        b,
        (((1,), (0,)), ((), ())),
        precision=lax.Precision.HIGHEST,
        preferred_element_type=jnp.float32,
    )


def kernel(
    n_high,
    n_low,
    blocks,
    rows,
    chunks,
    wave,
    level,
    phase,
    mix,
    out,
    lane_tab,
    row_tab,
    work,
    s1,
    r1,
    s2,
    r2,
    lv,
    trig,
    send_lv,
    recv_lv,
    send1,
    recv1,
    send2,
    recv2,
):
    group = n_high * n_low
    lanes = wave.shape[-1]
    total = blocks * rows
    piece = total // group
    rc = piece // chunks
    me = lax.axis_index("high") * n_low + lax.axis_index("low")

    def peer(k):
        return lax.rem(me + k, group)

    def where_is(other):
        return {"high": other // n_low, "low": lax.rem(other, n_low)}

    barrier = pltpu.get_barrier_semaphore()
    for k in range(1, group):
        pl.semaphore_signal(barrier, inc=1, device_id=where_is(peer(k)), device_id_type=MESH)

    mix_c, mix_s = cos_sin(mix[...])

    def angle(layer, g):
        return mix_c[layer : layer + 1, g : g + 1], mix_s[layer : layer + 1, g : g + 1]

    pl.semaphore_wait(barrier, group - 1)

    def level_copy(k):
        other = peer(k)
        return pltpu.make_async_remote_copy(
            src_ref=level.at[pl.ds(pl.multiple_of(other * piece, piece), piece)],
            dst_ref=lv.at[me],
            send_sem=send_lv.at[k],
            recv_sem=recv_lv.at[me],
            device_id=where_is(other),
            device_id_type=MESH,
        )

    def part_copy(source, target, send, recv, c, k):
        other = peer(k)
        return pltpu.make_async_remote_copy(
            src_ref=source.at[c, other],
            dst_ref=target.at[c, me],
            send_sem=send.at[c, k],
            recv_sem=recv.at[c, me],
            device_id=where_is(other),
            device_id_type=MESH,
        )

    def arrived(ref, sem, k):
        return pltpu.make_async_remote_copy(
            src_ref=ref,
            dst_ref=ref,
            send_sem=send_lv.at[k],
            recv_sem=sem,
            device_id=where_is(peer(k)),
            device_id_type=MESH,
        )

    for k in range(1, group):
        level_copy(k).start()

    for layer in range(LAYERS):
        lane_tab[layer] = rotation(lanes, *angle(layer, 0), True)
        row_tab[layer] = rotation(rows, *angle(layer, 1), False)

    step = min(16, rows)
    own_bits = popcount(me, bits_of(group))

    def quarter(row_start, count, block):
        row = lax.broadcasted_iota(jnp.int32, (count, lanes), 0) + row_start
        lane = lax.broadcasted_iota(jnp.int32, (count, lanes), 1)
        fixed = own_bits + block.bit_count()
        return (popcount(row, bits_of(rows)) + popcount(lane, bits_of(lanes)) + fixed) & 3

    def signs(q):
        one = jnp.float32(1.0)
        first = jnp.where((q == 1) | (q == 2), -one, one)
        second = jnp.where(q >= 2, -one, one)
        return (q & 1) == 1, first, second

    @pl.loop(0, rows // step)
    def _(n):
        start = pl.multiple_of(n * step, step)
        real, imag = [], []
        for b in range(blocks):
            at = pl.ds(b * rows + start, step)
            c, s = cos_sin(phase[0:1, :] * level[at, :])
            odd, first, second = signs(quarter(start, step, b))
            c, s = jnp.where(odd, s, c) * first, jnp.where(odd, c, s) * second
            u, v = wave[0, at, :], wave[1, at, :]
            real.append(u * c + v * s)
            imag.append(v * c - u * s)
        for bit in range(bits_of(blocks)):
            real = rotate_list(real, bit, *angle(0, 2))
            imag = rotate_list(imag, bit, *angle(0, 2))
        for b in range(blocks):
            at = pl.ds(b * rows + start, step)
            work[0, at, :] = real[b]
            work[1, at, :] = imag[b]

    lv[me] = level[pl.ds(pl.multiple_of(me * piece, piece), piece), :]

    per_block = rows // piece if piece <= rows else 0
    for part in range(2):
        for b in range(blocks):
            turned = mm(work[part, b * rows : (b + 1) * rows, :], lane_tab[0])
            turned = mm(row_tab[0], turned)
            for n in range(per_block):
                for c in range(chunks):
                    at = n * piece + c * rc
                    s1[c, b * per_block + n, part] = turned[at : at + rc]

    for c in range(chunks):
        r1[c, me] = s1[c, me]
        for k in range(1, group):
            part_copy(s1, r1, send1, recv1, c, k).start()

    for k in range(1, group):
        arrived(lv.at[peer(k)], recv_lv.at[peer(k)], k).wait_recv()

    @pl.loop(0, group)
    def _(g):
        c, s = cos_sin(phase[1:2, :] * lv[g])
        trig[0, g] = c
        trig[1, g] = s

    low_bits, all_bits = bits_of(n_low), bits_of(group)
    for c in range(chunks):
        for k in range(1, group):
            arrived(r1.at[c, peer(k)], recv1.at[c, peer(k)], k).wait_recv()

        @pl.loop(0, rc // 8)
        def _(n):
            at = pl.ds(pl.multiple_of(n * 8, 8), 8)
            from_piece = pl.ds(pl.multiple_of(c * rc + n * 8, 8), 8)
            real = [r1[c, g, 0, at, :] for g in range(group)]
            imag = [r1[c, g, 1, at, :] for g in range(group)]
            for bit in range(all_bits):
                turn = angle(0, 3 if bit < low_bits else 2)
                real = rotate_list(real, bit, *turn)
                imag = rotate_list(imag, bit, *turn)
            for g in range(group):
                co, si = trig[0, g, from_piece, :], trig[1, g, from_piece, :]
                u, v = real[g], imag[g]
                real[g] = u * co + v * si
                imag[g] = v * co - u * si
            for bit in range(all_bits):
                turn = angle(1, 3 if bit < low_bits else 2)
                real = rotate_list(real, bit, *turn)
                imag = rotate_list(imag, bit, *turn)
            for g in range(group):
                s2[c, g, 0, at, :] = real[g]
                s2[c, g, 1, at, :] = imag[g]

        r2[c, me] = s2[c, me]
        for k in range(1, group):
            part_copy(s2, r2, send2, recv2, c, k).start()

    for c in range(chunks):
        for k in range(1, group):
            arrived(r2.at[c, peer(k)], recv2.at[c, peer(k)], k).wait_recv()
        turned = mm(r2[c].reshape(group * 2 * rc, lanes), lane_tab[1])
        turned = turned.reshape(group, 2, rc, lanes)
        for g in range(group):
            for part in range(2):
                at = g * piece + c * rc
                work[part, at : at + rc, :] = turned[g, part]

    for part in range(2):
        for b in range(blocks):
            at = slice(b * rows, (b + 1) * rows)
            work[part, at, :] = mm(row_tab[1], work[part, at, :])

    @pl.loop(0, rows // step)
    def _(n):
        start = pl.multiple_of(n * step, step)
        spots = [pl.ds(b * rows + start, step) for b in range(blocks)]
        real = [work[0, at, :] for at in spots]
        imag = [work[1, at, :] for at in spots]
        for bit in range(bits_of(blocks)):
            real = rotate_list(real, bit, *angle(1, 2))
            imag = rotate_list(imag, bit, *angle(1, 2))
        for b in range(blocks):
            odd, first, second = signs(quarter(start, step, b))
            out[0, spots[b], :] = jnp.where(odd, imag[b], real[b]) * first
            out[1, spots[b], :] = jnp.where(odd, real[b], imag[b]) * second

    for k in range(1, group):
        level_copy(k).wait_send()
        for c in range(chunks):
            part_copy(s1, r1, send1, recv1, c, k).wait_send()
            part_copy(s2, r2, send2, recv2, c, k).wait_send()


def body(wave_parts, level_table, phase_angles, mix_angles):
    n_high, n_low = lax.axis_size("high"), lax.axis_size("low")
    group = n_high * n_low
    _, blocks, rows, lanes = wave_parts.shape
    total = blocks * rows
    piece = total // group
    chunks = max(1, min(CHUNKS, piece // 8))
    rc = piece // chunks
    parts = pltpu.VMEM((chunks, group, 2, rc, lanes), jnp.float32)
    vmem = pl.BlockSpec(memory_space=pltpu.VMEM)
    result = pl.pallas_call(
        functools.partial(kernel, n_high, n_low, blocks, rows, chunks),
        out_shape=jax.ShapeDtypeStruct((2, total, lanes), jnp.float32),
        in_specs=[vmem] * 4,
        out_specs=vmem,
        scratch_shapes=[
            pltpu.VMEM((LAYERS, lanes, lanes), jnp.float32),
            pltpu.VMEM((LAYERS, rows, rows), jnp.float32),
            pltpu.VMEM((2, total, lanes), jnp.float32),
            parts,
            parts,
            parts,
            parts,
            pltpu.VMEM((group, piece, lanes), jnp.float32),
            pltpu.VMEM((2, group, piece, lanes), jnp.float32),
            pltpu.SemaphoreType.DMA((group,)),
            pltpu.SemaphoreType.DMA((group,)),
            pltpu.SemaphoreType.DMA((chunks, group)),
            pltpu.SemaphoreType.DMA((chunks, group)),
            pltpu.SemaphoreType.DMA((chunks, group)),
            pltpu.SemaphoreType.DMA((chunks, group)),
        ],
        compiler_params=pltpu.CompilerParams(collective_id=0, has_side_effects=True),
    )(
        wave_parts.reshape(2, total, lanes),
        level_table.reshape(total, lanes),
        phase_angles,
        mix_angles,
    )
    return result.reshape(wave_parts.shape)


def solution(mesh):
    placed = (
        P("unit", ("high", "low"), None, None),
        P(("unit", "high", "low"), None, None),
        P("unit", None),
        P("unit", None),
    )
    return jax.shard_map(
        body,
        mesh=mesh,
        in_specs=placed,
        out_specs=P("unit", ("high", "low"), None, None),
        check_vma=False,
    )
```

```python
import functools
import math

import jax
import jax.numpy as jnp
from jax import lax
from jax.experimental import pallas as pl
from jax.experimental.pallas import tpu as pltpu
from jax.sharding import PartitionSpec as P

LAYERS = 2
MESH = pl.DeviceIdType.MESH
CHUNKS = 4


def cos_sin(x):
    turns = jnp.floor(x * (0.5 / math.pi) + 0.5)
    r = x - turns * 6.28125
    r = r - turns * (2 * math.pi - 6.28125)
    y = r * r
    sine = jnp.full_like(y, -1.0 / math.factorial(19))
    for n in range(17, 0, -2):
        sine = sine * y + (-1.0) ** (n // 2) / math.factorial(n)
    cosine = jnp.full_like(y, -1.0 / math.factorial(18))
    for n in range(16, -1, -2):
        cosine = cosine * y + (-1.0) ** (n // 2) / math.factorial(n)
    return cosine, sine * r


def bits_of(count):
    return count.bit_length() - 1


def popcount(values, bits):
    total = values & 1
    for k in range(1, bits):
        total = total + ((values >> k) & 1)
    return total


def rotation(size, c, s, transposed):
    out = lax.broadcasted_iota(jnp.int32, (size, size), 1 if transposed else 0)
    inn = lax.broadcasted_iota(jnp.int32, (size, size), 0 if transposed else 1)
    differ = out ^ inn
    c = jnp.broadcast_to(c, (size, size))
    s = jnp.broadcast_to(s, (size, size))
    table = None
    for k in range(bits_of(size)):
        turned = jnp.where(((out >> k) & 1) == 1, -s, s)
        factor = jnp.where(((differ >> k) & 1) == 1, turned, c)
        table = factor if table is None else table * factor
    return table


def rotate_list(parts, bit, c, s):
    fresh = list(parts)
    for n in range(len(parts)):
        if not n >> bit & 1:
            m = n | 1 << bit
            fresh[n] = c * parts[n] + s * parts[m]
            fresh[m] = c * parts[m] - s * parts[n]
    return fresh


def halves(values):
    high = values.astype(jnp.bfloat16)
    return high, (values - high.astype(jnp.float32)).astype(jnp.bfloat16)


def lane_table(table):
    pair = jnp.concatenate(halves(table), axis=1)
    return jnp.concatenate([pair, pair], axis=0)


def row_table(table):
    pair = jnp.concatenate(halves(table), axis=0)
    return jnp.concatenate([pair, pair], axis=1)


def by_lane(values, table):
    wide = jnp.concatenate(halves(values), axis=1)
    sums = jnp.dot(wide, table, preferred_element_type=jnp.float32)
    lanes = values.shape[1]
    return sums[:, :lanes] + sums[:, lanes:]


def by_row(table, values):
    tall = jnp.concatenate(halves(values), axis=0)
    sums = jnp.dot(table, tall, preferred_element_type=jnp.float32)
    rows = values.shape[0]
    return sums[:rows] + sums[rows:]


def kernel(
    n_high,
    n_low,
    blocks,
    rows,
    chunks,
    wave,
    level,
    phase,
    mix,
    out,
    lane_tab,
    row_tab,
    work,
    mid,
    s1,
    r1,
    s2,
    r2,
    lv,
    trig,
    send_lv,
    recv_lv,
    send1,
    recv1,
    send2,
    recv2,
):
    group = n_high * n_low
    lanes = wave.shape[-1]
    total = blocks * rows
    piece = total // group
    rc = piece // chunks
    me = lax.axis_index("high") * n_low + lax.axis_index("low")

    def peer(k):
        return lax.rem(me + k, group)

    def where_is(other):
        return {"high": other // n_low, "low": lax.rem(other, n_low)}

    barrier = pltpu.get_barrier_semaphore()
    for k in range(1, group):
        pl.semaphore_signal(barrier, inc=1, device_id=where_is(peer(k)), device_id_type=MESH)

    mix_c, mix_s = cos_sin(mix[...])

    def angle(layer, g):
        return mix_c[layer : layer + 1, g : g + 1], mix_s[layer : layer + 1, g : g + 1]

    pl.semaphore_wait(barrier, group - 1)

    def level_copy(k):
        other = peer(k)
        return pltpu.make_async_remote_copy(
            src_ref=level.at[pl.ds(pl.multiple_of(other * piece, piece), piece)],
            dst_ref=lv.at[me],
            send_sem=send_lv.at[k],
            recv_sem=recv_lv.at[me],
            device_id=where_is(other),
            device_id_type=MESH,
        )

    def part_copy(source, target, send, recv, c, k):
        other = peer(k)
        return pltpu.make_async_remote_copy(
            src_ref=source.at[c, other],
            dst_ref=target.at[c, me],
            send_sem=send.at[c, k],
            recv_sem=recv.at[c, me],
            device_id=where_is(other),
            device_id_type=MESH,
        )

    def arrived(ref, sem, k):
        return pltpu.make_async_remote_copy(
            src_ref=ref,
            dst_ref=ref,
            send_sem=send_lv.at[k],
            recv_sem=sem,
            device_id=where_is(peer(k)),
            device_id_type=MESH,
        )

    for k in range(1, group):
        level_copy(k).start()

    for layer in range(LAYERS):
        lane_tab[layer] = lane_table(rotation(lanes, *angle(layer, 0), True))
        row_tab[layer] = row_table(rotation(rows, *angle(layer, 1), False))

    step = min(16, rows)
    own_bits = popcount(me, bits_of(group))

    def quarter(row_start, count, block):
        row = lax.broadcasted_iota(jnp.int32, (count, lanes), 0) + row_start
        lane = lax.broadcasted_iota(jnp.int32, (count, lanes), 1)
        fixed = own_bits + block.bit_count()
        return (popcount(row, bits_of(rows)) + popcount(lane, bits_of(lanes)) + fixed) & 3

    def signs(q):
        one = jnp.float32(1.0)
        first = jnp.where((q == 1) | (q == 2), -one, one)
        second = jnp.where(q >= 2, -one, one)
        return (q & 1) == 1, first, second

    @pl.loop(0, rows // step)
    def _(n):
        start = pl.multiple_of(n * step, step)
        real, imag = [], []
        for b in range(blocks):
            at = pl.ds(b * rows + start, step)
            c, s = cos_sin(phase[0:1, :] * level[at, :])
            odd, first, second = signs(quarter(start, step, b))
            c, s = jnp.where(odd, s, c) * first, jnp.where(odd, c, s) * second
            u, v = wave[0, at, :], wave[1, at, :]
            real.append(u * c + v * s)
            imag.append(v * c - u * s)
        for bit in range(bits_of(blocks)):
            real = rotate_list(real, bit, *angle(0, 2))
            imag = rotate_list(imag, bit, *angle(0, 2))
        for b in range(blocks):
            at = pl.ds(b * rows + start, step)
            work[0, at, :] = real[b]
            work[1, at, :] = imag[b]

    lv[me] = level[pl.ds(pl.multiple_of(me * piece, piece), piece), :]

    per_block = rows // piece if piece <= rows else 0
    for b in range(blocks):
        at = slice(b * rows, (b + 1) * rows)
        turned = by_row(row_tab[0], jnp.concatenate([work[0, at, :], work[1, at, :]], axis=1))
        for part in range(2):
            for n in range(per_block):
                for c in range(chunks):
                    at = n * piece + c * rc
                    s1[c, b * per_block + n, part] = turned[
                        at : at + rc, part * lanes : (part + 1) * lanes
                    ]

    for c in range(chunks):
        r1[c, me] = s1[c, me]
        for k in range(1, group):
            part_copy(s1, r1, send1, recv1, c, k).start()

    for k in range(1, group):
        arrived(lv.at[peer(k)], recv_lv.at[peer(k)], k).wait_recv()

    @pl.loop(0, group)
    def _(g):
        c, s = cos_sin(phase[1:2, :] * lv[g])
        trig[0, g] = c
        trig[1, g] = s

    low_bits, all_bits = bits_of(n_low), bits_of(group)
    for c in range(chunks):
        for k in range(1, group):
            arrived(r1.at[c, peer(k)], recv1.at[c, peer(k)], k).wait_recv()

        tall = group * 2 * rc
        turned = by_lane(r1[c].reshape(tall, lanes), lane_tab[0])
        mid[...] = turned.reshape(group, 2, rc, lanes)

        @pl.loop(0, rc // 8)
        def _(n):
            at = pl.ds(pl.multiple_of(n * 8, 8), 8)
            from_piece = pl.ds(pl.multiple_of(c * rc + n * 8, 8), 8)
            real = [mid[g, 0, at, :] for g in range(group)]
            imag = [mid[g, 1, at, :] for g in range(group)]
            for bit in range(all_bits):
                turn = angle(0, 3 if bit < low_bits else 2)
                real = rotate_list(real, bit, *turn)
                imag = rotate_list(imag, bit, *turn)
            for g in range(group):
                co, si = trig[0, g, from_piece, :], trig[1, g, from_piece, :]
                u, v = real[g], imag[g]
                real[g] = u * co + v * si
                imag[g] = v * co - u * si
            for bit in range(all_bits):
                turn = angle(1, 3 if bit < low_bits else 2)
                real = rotate_list(real, bit, *turn)
                imag = rotate_list(imag, bit, *turn)
            for g in range(group):
                mid[g, 0, at, :] = real[g]
                mid[g, 1, at, :] = imag[g]

        turned = by_lane(mid[...].reshape(tall, lanes), lane_tab[1])
        s2[c] = turned.reshape(group, 2, rc, lanes)
        r2[c, me] = s2[c, me]
        for k in range(1, group):
            part_copy(s2, r2, send2, recv2, c, k).start()

    for c in range(chunks):
        for k in range(1, group):
            arrived(r2.at[c, peer(k)], recv2.at[c, peer(k)], k).wait_recv()
        for g in range(group):
            for part in range(2):
                at = g * piece + c * rc
                work[part, at : at + rc, :] = r2[c, g, part]

    for b in range(blocks):
        at = slice(b * rows, (b + 1) * rows)
        turned = by_row(row_tab[1], jnp.concatenate([work[0, at, :], work[1, at, :]], axis=1))
        work[0, at, :] = turned[:, :lanes]
        work[1, at, :] = turned[:, lanes:]

    @pl.loop(0, rows // step)
    def _(n):
        start = pl.multiple_of(n * step, step)
        spots = [pl.ds(b * rows + start, step) for b in range(blocks)]
        real = [work[0, at, :] for at in spots]
        imag = [work[1, at, :] for at in spots]
        for bit in range(bits_of(blocks)):
            real = rotate_list(real, bit, *angle(1, 2))
            imag = rotate_list(imag, bit, *angle(1, 2))
        for b in range(blocks):
            odd, first, second = signs(quarter(start, step, b))
            out[0, spots[b], :] = jnp.where(odd, imag[b], real[b]) * first
            out[1, spots[b], :] = jnp.where(odd, real[b], imag[b]) * second

    for k in range(1, group):
        level_copy(k).wait_send()
        for c in range(chunks):
            part_copy(s1, r1, send1, recv1, c, k).wait_send()
            part_copy(s2, r2, send2, recv2, c, k).wait_send()


def body(wave_parts, level_table, phase_angles, mix_angles):
    n_high, n_low = lax.axis_size("high"), lax.axis_size("low")
    group = n_high * n_low
    _, blocks, rows, lanes = wave_parts.shape
    total = blocks * rows
    piece = total // group
    chunks = max(1, min(CHUNKS, piece // 8))
    rc = piece // chunks
    parts = pltpu.VMEM((chunks, group, 2, rc, lanes), jnp.float32)
    vmem = pl.BlockSpec(memory_space=pltpu.VMEM)
    result = pl.pallas_call(
        functools.partial(kernel, n_high, n_low, blocks, rows, chunks),
        out_shape=jax.ShapeDtypeStruct((2, total, lanes), jnp.float32),
        in_specs=[vmem] * 4,
        out_specs=vmem,
        scratch_shapes=[
            pltpu.VMEM((LAYERS, 2 * lanes, 2 * lanes), jnp.bfloat16),
            pltpu.VMEM((LAYERS, 2 * rows, 2 * rows), jnp.bfloat16),
            pltpu.VMEM((2, total, lanes), jnp.float32),
            pltpu.VMEM((group, 2, rc, lanes), jnp.float32),
            parts,
            parts,
            parts,
            parts,
            pltpu.VMEM((group, piece, lanes), jnp.float32),
            pltpu.VMEM((2, group, piece, lanes), jnp.float32),
            pltpu.SemaphoreType.DMA((group,)),
            pltpu.SemaphoreType.DMA((group,)),
            pltpu.SemaphoreType.DMA((chunks, group)),
            pltpu.SemaphoreType.DMA((chunks, group)),
            pltpu.SemaphoreType.DMA((chunks, group)),
            pltpu.SemaphoreType.DMA((chunks, group)),
        ],
        compiler_params=pltpu.CompilerParams(collective_id=0, has_side_effects=True),
    )(
        wave_parts.reshape(2, total, lanes),
        level_table.reshape(total, lanes),
        phase_angles,
        mix_angles,
    )
    return result.reshape(wave_parts.shape)


def solution(mesh):
    placed = (
        P("unit", ("high", "low"), None, None),
        P(("unit", "high", "low"), None, None),
        P("unit", None),
        P("unit", None),
    )
    return jax.shard_map(
        body,
        mesh=mesh,
        in_specs=placed,
        out_specs=P("unit", ("high", "low"), None, None),
        check_vma=False,
    )
```

```python
import functools
import math

import jax
import jax.numpy as jnp
from jax import lax
from jax.experimental import pallas as pl
from jax.experimental.pallas import tpu as pltpu
from jax.sharding import PartitionSpec as P

LAYERS = 2
MESH = pl.DeviceIdType.MESH
CHUNKS = 2


def cos_sin(x):
    turns = jnp.floor(x * (0.5 / math.pi) + 0.5)
    r = x - turns * 6.28125
    r = r - turns * (2 * math.pi - 6.28125)
    y = r * r
    sine = jnp.full_like(y, -1.0 / math.factorial(19))
    for n in range(17, 0, -2):
        sine = sine * y + (-1.0) ** (n // 2) / math.factorial(n)
    cosine = jnp.full_like(y, -1.0 / math.factorial(18))
    for n in range(16, -1, -2):
        cosine = cosine * y + (-1.0) ** (n // 2) / math.factorial(n)
    return cosine, sine * r


def bits_of(count):
    return count.bit_length() - 1


def popcount(values, bits):
    total = values & 1
    for k in range(1, bits):
        total = total + ((values >> k) & 1)
    return total


def rotation(size, c, s, transposed):
    out = lax.broadcasted_iota(jnp.int32, (size, size), 1 if transposed else 0)
    inn = lax.broadcasted_iota(jnp.int32, (size, size), 0 if transposed else 1)
    differ = out ^ inn
    c = jnp.broadcast_to(c, (size, size))
    s = jnp.broadcast_to(s, (size, size))
    table = None
    for k in range(bits_of(size)):
        turned = jnp.where(((out >> k) & 1) == 1, -s, s)
        factor = jnp.where(((differ >> k) & 1) == 1, turned, c)
        table = factor if table is None else table * factor
    return table


def rotate_list(parts, bit, c, s):
    fresh = list(parts)
    for n in range(len(parts)):
        if not n >> bit & 1:
            m = n | 1 << bit
            fresh[n] = c * parts[n] + s * parts[m]
            fresh[m] = c * parts[m] - s * parts[n]
    return fresh


def halves(values):
    high = values.astype(jnp.bfloat16)
    return high, (values - high.astype(jnp.float32)).astype(jnp.bfloat16)


def lane_table(table):
    pair = jnp.concatenate(halves(table), axis=1)
    return jnp.concatenate([pair, pair], axis=0)


def row_table(table):
    pair = jnp.concatenate(halves(table), axis=0)
    return jnp.concatenate([pair, pair], axis=1)


def by_lane(values, table):
    wide = jnp.concatenate(halves(values), axis=1)
    sums = jnp.dot(wide, table, preferred_element_type=jnp.float32)
    lanes = values.shape[1]
    return sums[:, :lanes] + sums[:, lanes:]


def by_row(table, values):
    tall = jnp.concatenate(halves(values), axis=0)
    sums = jnp.dot(table, tall, preferred_element_type=jnp.float32)
    rows = values.shape[0]
    return sums[:rows] + sums[rows:]


def kernel(
    n_high,
    n_low,
    blocks,
    rows,
    chunks,
    wave,
    level,
    phase,
    mix,
    out,
    lane_tab,
    row_tab,
    work,
    mid,
    s1,
    r1,
    s2,
    r2,
    lv,
    trig,
    send_lv,
    recv_lv,
    send1,
    recv1,
    send2,
    recv2,
):
    group = n_high * n_low
    lanes = wave.shape[-1]
    total = blocks * rows
    piece = total // group
    rc = piece // chunks
    me = lax.axis_index("high") * n_low + lax.axis_index("low")

    def peer(k):
        return lax.rem(me + k, group)

    def where_is(other):
        return {"high": other // n_low, "low": lax.rem(other, n_low)}

    barrier = pltpu.get_barrier_semaphore()
    for k in range(1, group):
        pl.semaphore_signal(barrier, inc=1, device_id=where_is(peer(k)), device_id_type=MESH)

    mix_c, mix_s = cos_sin(mix[...])

    def angle(layer, g):
        return mix_c[layer : layer + 1, g : g + 1], mix_s[layer : layer + 1, g : g + 1]

    pl.semaphore_wait(barrier, group - 1)

    def level_copy(k):
        other = peer(k)
        return pltpu.make_async_remote_copy(
            src_ref=level.at[pl.ds(pl.multiple_of(other * piece, piece), piece)],
            dst_ref=lv.at[me],
            send_sem=send_lv.at[k],
            recv_sem=recv_lv.at[me],
            device_id=where_is(other),
            device_id_type=MESH,
        )

    def part_copy(source, target, send, recv, c, k):
        other = peer(k)
        return pltpu.make_async_remote_copy(
            src_ref=source.at[c, other],
            dst_ref=target.at[c, me],
            send_sem=send.at[c, k],
            recv_sem=recv.at[c, me],
            device_id=where_is(other),
            device_id_type=MESH,
        )

    def arrived(ref, sem, k):
        return pltpu.make_async_remote_copy(
            src_ref=ref,
            dst_ref=ref,
            send_sem=send_lv.at[k],
            recv_sem=sem,
            device_id=where_is(peer(k)),
            device_id_type=MESH,
        )

    for k in range(1, group):
        level_copy(k).start()

    for layer in range(LAYERS):
        lane_tab[layer] = lane_table(rotation(lanes, *angle(layer, 0), True))
        row_tab[layer] = row_table(rotation(rows, *angle(layer, 1), False))

    step = min(16, rows)
    own_bits = popcount(me, bits_of(group))

    def quarter(row_start, count, block):
        row = lax.broadcasted_iota(jnp.int32, (count, lanes), 0) + row_start
        lane = lax.broadcasted_iota(jnp.int32, (count, lanes), 1)
        fixed = own_bits + block.bit_count()
        return (popcount(row, bits_of(rows)) + popcount(lane, bits_of(lanes)) + fixed) & 3

    def signs(q):
        one = jnp.float32(1.0)
        first = jnp.where((q == 1) | (q == 2), -one, one)
        second = jnp.where(q >= 2, -one, one)
        return (q & 1) == 1, first, second

    @pl.loop(0, rows // step)
    def _(n):
        start = pl.multiple_of(n * step, step)
        real, imag = [], []
        for b in range(blocks):
            at = pl.ds(b * rows + start, step)
            c, s = cos_sin(phase[0:1, :] * level[at, :])
            odd, first, second = signs(quarter(start, step, b))
            c, s = jnp.where(odd, s, c) * first, jnp.where(odd, c, s) * second
            u, v = wave[0, at, :], wave[1, at, :]
            real.append(u * c + v * s)
            imag.append(v * c - u * s)
        for bit in range(bits_of(blocks)):
            real = rotate_list(real, bit, *angle(0, 2))
            imag = rotate_list(imag, bit, *angle(0, 2))
        for b in range(blocks):
            at = pl.ds(b * rows + start, step)
            work[0, at, :] = real[b]
            work[1, at, :] = imag[b]

    lv[me] = level[pl.ds(pl.multiple_of(me * piece, piece), piece), :]

    per_block = rows // piece if piece <= rows else 0
    for b in range(blocks):
        at = slice(b * rows, (b + 1) * rows)
        turned = by_row(row_tab[0], jnp.concatenate([work[0, at, :], work[1, at, :]], axis=1))
        for part in range(2):
            for n in range(per_block):
                for c in range(chunks):
                    at = n * piece + c * rc
                    s1[c, b * per_block + n, part] = turned[
                        at : at + rc, part * lanes : (part + 1) * lanes
                    ]

    for c in range(chunks):
        r1[c, me] = s1[c, me]
        for k in range(1, group):
            part_copy(s1, r1, send1, recv1, c, k).start()

    for k in range(1, group):
        arrived(lv.at[peer(k)], recv_lv.at[peer(k)], k).wait_recv()

    @pl.loop(0, group)
    def _(g):
        c, s = cos_sin(phase[1:2, :] * lv[g])
        trig[0, g] = c
        trig[1, g] = s

    low_bits, all_bits = bits_of(n_low), bits_of(group)
    for c in range(chunks):
        for k in range(1, group):
            arrived(r1.at[c, peer(k)], recv1.at[c, peer(k)], k).wait_recv()

        tall = group * 2 * rc
        turned = by_lane(r1[c].reshape(tall, lanes), lane_tab[0])
        mid[...] = turned.reshape(group, 2, rc, lanes)

        @pl.loop(0, rc // 8)
        def _(n):
            at = pl.ds(pl.multiple_of(n * 8, 8), 8)
            from_piece = pl.ds(pl.multiple_of(c * rc + n * 8, 8), 8)
            real = [mid[g, 0, at, :] for g in range(group)]
            imag = [mid[g, 1, at, :] for g in range(group)]
            for bit in range(all_bits):
                turn = angle(0, 3 if bit < low_bits else 2)
                real = rotate_list(real, bit, *turn)
                imag = rotate_list(imag, bit, *turn)
            for g in range(group):
                co, si = trig[0, g, from_piece, :], trig[1, g, from_piece, :]
                u, v = real[g], imag[g]
                real[g] = u * co + v * si
                imag[g] = v * co - u * si
            for bit in range(all_bits):
                turn = angle(1, 3 if bit < low_bits else 2)
                real = rotate_list(real, bit, *turn)
                imag = rotate_list(imag, bit, *turn)
            for g in range(group):
                mid[g, 0, at, :] = real[g]
                mid[g, 1, at, :] = imag[g]

        turned = by_lane(mid[...].reshape(tall, lanes), lane_tab[1])
        s2[c] = turned.reshape(group, 2, rc, lanes)
        r2[c, me] = s2[c, me]
        for k in range(1, group):
            part_copy(s2, r2, send2, recv2, c, k).start()

    for c in range(chunks):
        for k in range(1, group):
            arrived(r2.at[c, peer(k)], recv2.at[c, peer(k)], k).wait_recv()
        for g in range(group):
            for part in range(2):
                at = g * piece + c * rc
                work[part, at : at + rc, :] = r2[c, g, part]

    for b in range(blocks):
        at = slice(b * rows, (b + 1) * rows)
        turned = by_row(row_tab[1], jnp.concatenate([work[0, at, :], work[1, at, :]], axis=1))
        work[0, at, :] = turned[:, :lanes]
        work[1, at, :] = turned[:, lanes:]

    @pl.loop(0, rows // step)
    def _(n):
        start = pl.multiple_of(n * step, step)
        spots = [pl.ds(b * rows + start, step) for b in range(blocks)]
        real = [work[0, at, :] for at in spots]
        imag = [work[1, at, :] for at in spots]
        for bit in range(bits_of(blocks)):
            real = rotate_list(real, bit, *angle(1, 2))
            imag = rotate_list(imag, bit, *angle(1, 2))
        for b in range(blocks):
            odd, first, second = signs(quarter(start, step, b))
            out[0, spots[b], :] = jnp.where(odd, imag[b], real[b]) * first
            out[1, spots[b], :] = jnp.where(odd, real[b], imag[b]) * second

    for k in range(1, group):
        level_copy(k).wait_send()
        for c in range(chunks):
            part_copy(s1, r1, send1, recv1, c, k).wait_send()
            part_copy(s2, r2, send2, recv2, c, k).wait_send()


def body(wave_parts, level_table, phase_angles, mix_angles):
    n_high, n_low = lax.axis_size("high"), lax.axis_size("low")
    group = n_high * n_low
    _, blocks, rows, lanes = wave_parts.shape
    total = blocks * rows
    piece = total // group
    chunks = max(1, min(CHUNKS, piece // 8))
    rc = piece // chunks
    parts = pltpu.VMEM((chunks, group, 2, rc, lanes), jnp.float32)
    vmem = pl.BlockSpec(memory_space=pltpu.VMEM)
    result = pl.pallas_call(
        functools.partial(kernel, n_high, n_low, blocks, rows, chunks),
        out_shape=jax.ShapeDtypeStruct((2, total, lanes), jnp.float32),
        in_specs=[vmem] * 4,
        out_specs=vmem,
        scratch_shapes=[
            pltpu.VMEM((LAYERS, 2 * lanes, 2 * lanes), jnp.bfloat16),
            pltpu.VMEM((LAYERS, 2 * rows, 2 * rows), jnp.bfloat16),
            pltpu.VMEM((2, total, lanes), jnp.float32),
            pltpu.VMEM((group, 2, rc, lanes), jnp.float32),
            parts,
            parts,
            parts,
            parts,
            pltpu.VMEM((group, piece, lanes), jnp.float32),
            pltpu.VMEM((2, group, piece, lanes), jnp.float32),
            pltpu.SemaphoreType.DMA((group,)),
            pltpu.SemaphoreType.DMA((group,)),
            pltpu.SemaphoreType.DMA((chunks, group)),
            pltpu.SemaphoreType.DMA((chunks, group)),
            pltpu.SemaphoreType.DMA((chunks, group)),
            pltpu.SemaphoreType.DMA((chunks, group)),
        ],
        compiler_params=pltpu.CompilerParams(collective_id=0, has_side_effects=True),
    )(
        wave_parts.reshape(2, total, lanes),
        level_table.reshape(total, lanes),
        phase_angles,
        mix_angles,
    )
    return result.reshape(wave_parts.shape)


def solution(mesh):
    placed = (
        P("unit", ("high", "low"), None, None),
        P(("unit", "high", "low"), None, None),
        P("unit", None),
        P("unit", None),
    )
    return jax.shard_map(
        body,
        mesh=mesh,
        in_specs=placed,
        out_specs=P("unit", ("high", "low"), None, None),
        check_vma=False,
    )
```
